32 devices in a mesh: seq: 4 (over y, core), blk: 8 (over z, x).
Axes of the slice: x: 2, y: 2, z: 4, core: 2. Of those that a mesh axis runs over, the one named last changes fastest.
Arguments:
- kv_cache: bfloat16 [4, 2, 16, 4096, 1024], P(None, None, None, ('seq', 'blk')), may hold values from -18 to 18, as said below
- queries: bfloat16 [4, 128, 1024], P(None, 'blk'), may hold values from -400 to 400
- fresh_key_value: bfloat16 [4, 2, 128, 128], P(None, None, 'blk'), may hold values from -70 to 70
- lengths: int32 [16], replicated, may hold values from 1 to 4096, 49152 in all
Outputs:
- quant_cache: bfloat16 [4, 2, 128, 4096, 128], P(None, None, 'blk', 'seq')
- block_scale: float32 [4, 2, 128, 32], P(None, None, 'blk', 'seq')
- attended: bfloat16 [4, 128, 1024], P(None, 'blk')
The draws below stay inside these ranges and needn't reach their ends.
Inputs may be any that keep to these rules, and one draw needn't show every extreme that they name: `kv_cache`: each entry is a random value times a factor drawn for its position and head. `lengths`: every sequence has at least one live position, and some sequence uses all 4096.
All inputs are finite; a program needn't handle non-finite values.
Results may differ from the reference program's by a relative error of at most 0.003.
The reference program's roundings to bfloat16 on the way count: a program that leaves them out, or rounds other values in their place, can miss the bound.
Values may be sent and summed in bfloat16 or wider, within the bound.
No kernel may reach another device: no remote copies, remote signals or barrier semaphores. Data moves between devices by JAX's collectives and lax.ppermute only.
A program may use at most 192 MiB of HBM per device.

```python
import math
import jax
import jax.numpy as jnp
import numpy as np
from jax import lax

KEY_VALUE_HEADS = 8
HEAD_DIM = 128
QUERY_GROUP = 8
SEQUENCE_COUNT = 16
CACHE_LENGTH = 4096
LAYER_COUNT = 4
BLOCK = 128


def draw_kv_cache(key, part):
    first_part, second_part = jax.random.split(jax.random.fold_in(key, 11))
    array_shape = (LAYER_COUNT, 2, SEQUENCE_COUNT, CACHE_LENGTH, KEY_VALUE_HEADS, HEAD_DIM)
    base_offset = jax.random.truncated_normal(first_part, -4.0, 4.0, array_shape, jnp.float32)
    scale_factor = jnp.exp(jax.random.uniform(second_part, (LAYER_COUNT, 2, SEQUENCE_COUNT, CACHE_LENGTH, KEY_VALUE_HEADS, 1), jnp.float32, -1.5, 1.5))
    return (base_offset * scale_factor).reshape(LAYER_COUNT, 2, SEQUENCE_COUNT, CACHE_LENGTH, KEY_VALUE_HEADS * HEAD_DIM).astype(jnp.bfloat16)


def draw_queries(key, part):
    first_part, second_part = jax.random.split(jax.random.fold_in(key, 23))
    base_offset = jax.random.truncated_normal(first_part, -6.0, 6.0, (LAYER_COUNT, KEY_VALUE_HEADS * SEQUENCE_COUNT, QUERY_GROUP, HEAD_DIM), jnp.float32)
    return base_offset.reshape(LAYER_COUNT, KEY_VALUE_HEADS * SEQUENCE_COUNT, QUERY_GROUP * HEAD_DIM).astype(jnp.bfloat16)


def draw_fresh_key_value(key, part):
    noise_key, value_key = jax.random.split(jax.random.fold_in(key, 37))
    query_rows = draw_queries(key, part).astype(jnp.float32)
    query_rows = query_rows.reshape(LAYER_COUNT, KEY_VALUE_HEADS * SEQUENCE_COUNT, QUERY_GROUP, HEAD_DIM)
    summed = jnp.sum(query_rows, axis=2)
    length = jnp.sqrt(jnp.sum(summed * summed, axis=-1, keepdims=True) + 1.0)
    noise = 0.5 * jax.random.normal(noise_key, summed.shape, jnp.float32)
    fresh_key = jnp.clip(5.0 * jnp.sqrt(jnp.float32(HEAD_DIM)) * summed / length + noise, -70.0, 70.0)
    fresh_value = jax.random.truncated_normal(value_key, -6.0, 6.0, summed.shape, jnp.float32)
    return jnp.stack([fresh_key, fresh_value], axis=1).astype(jnp.bfloat16)


def length_profile(number_of, total, limit, skew):
    weights = [(1 << 20) // math.isqrt(rank ** skew) + 1 for rank in range(2, number_of + 1)]
    spare, counts = total - limit - (number_of - 1), [1] * (number_of - 1)
    while spare > 0:
        candidates = [i for i in range(number_of - 1) if counts[i] < limit]
        pool, left = sum([weights[i] for i in candidates]), spare
        for i in candidates:
            more = min(limit - counts[i], max(1, left * weights[i] // pool), spare)
            counts[i] = counts[i] + more
            spare = spare - more
    return np.array([limit] + counts)


def ragged(stream_key, amount, total, reach, slope):
    if amount == 2:
        one = jax.random.randint(stream_key, (), max(1, total - reach), min(reach, total - 1) + 1)
        return jnp.stack([one, total - one])
    tallies = jnp.asarray(length_profile(amount, total, reach, slope), jnp.int32)
    pairs = (amount - 1) // 2
    source_of, taker = tallies[1:1 + 2 * pairs:2], tallies[2:2 + 2 * pairs:2]
    margin = jnp.minimum(source_of - 1, reach - taker)
    moved = jax.random.randint(jax.random.fold_in(stream_key, 1), (pairs,), 0, 1 << 20) % (margin + 1)
    tallies = tallies.at[1:1 + 2 * pairs:2].set(source_of - moved).at[2:2 + 2 * pairs:2].set(taker + moved)
    return tallies[jax.random.permutation(jax.random.fold_in(stream_key, 2), amount)]


def setup_inputs(seed: int = 0) -> dict:
    key_list = jax.random.split(jax.random.key(seed), 5)
    return {
        "kv_cache": draw_kv_cache(jax.random.fold_in(key_list[4], 71), 0),
        "queries": draw_queries(jax.random.fold_in(key_list[4], 71), 0),
        "fresh_key_value": draw_fresh_key_value(jax.random.fold_in(key_list[4], 71), 0),
        "lengths": ragged(key_list[3], SEQUENCE_COUNT, 3 * SEQUENCE_COUNT * CACHE_LENGTH // 4, CACHE_LENGTH, 1).astype(jnp.int32),
    }


def one_layer(lengths, items):
    cache, query, fresh = items
    seq_len = cache.shape[2]
    batch = cache.shape[1]
    heads = cache.shape[3] // HEAD_DIM
    blocks = seq_len // BLOCK
    values = cache.astype(jnp.float32).reshape(2, batch, blocks, BLOCK, heads, HEAD_DIM)
    scale = jnp.maximum(lax.optimization_barrier(jnp.max(jnp.abs(values), axis=(3, 5))), 1.0) / 127.0
    quant = (values / scale[:, :, :, None, :, None]).astype(jnp.bfloat16)
    quant = quant.transpose(0, 4, 1, 2, 3, 5).reshape(2, heads * batch, seq_len, HEAD_DIM)
    scale = scale.transpose(0, 3, 1, 2).reshape(2, heads * batch, blocks)
    rows = heads * batch
    inverse = 1.0 / jnp.sqrt(jnp.float32(HEAD_DIM))
    grouped = query.reshape(rows, QUERY_GROUP, HEAD_DIM).astype(jnp.float32)
    raw = jnp.einsum('pgd,prd->pgr', grouped, quant[0].astype(jnp.float32), precision=lax.Precision.HIGHEST)
    scores = raw.reshape(rows, QUERY_GROUP, blocks, BLOCK) * scale[0][:, None, :, None] * inverse
    pair_len = jnp.tile(lengths, heads)
    positions = jnp.arange(seq_len, dtype=jnp.int32).reshape(blocks, BLOCK)
    valid = positions[None] < pair_len[:, None, None]
    masked = jnp.where(valid[:, None], scores, -1e+30)
    peak = lax.optimization_barrier(jnp.max(masked, axis=-1))
    weight = jnp.where(valid[:, None], jnp.exp(masked - peak[..., None]), 0.0)
    total = lax.optimization_barrier(jnp.sum(weight, axis=-1))
    rounded = (weight * scale[1][:, None, :, None]).astype(jnp.bfloat16)
    part = jnp.einsum('pgnt,pntd->pgnd', rounded.astype(jnp.float32), quant[1].reshape(rows, blocks, BLOCK, HEAD_DIM).astype(jnp.float32), precision=lax.Precision.HIGHEST)
    own = jnp.einsum('pgd,pd->pg', grouped, fresh[0].astype(jnp.float32), precision=lax.Precision.HIGHEST) * inverse
    top = jnp.maximum(lax.optimization_barrier(jnp.max(peak, axis=-1)), own)
    scale_factor = jnp.exp(peak - top[..., None])
    own_w = jnp.exp(own - top)
    numer = lax.optimization_barrier(jnp.sum(scale_factor[..., None] * part, axis=2)) + own_w[..., None] * fresh[1].astype(jnp.float32)[:, None, :]
    denom = lax.optimization_barrier(jnp.sum(scale_factor * total, axis=-1)) + own_w
    attended = (numer / denom[..., None]).reshape(rows, QUERY_GROUP * HEAD_DIM).astype(jnp.bfloat16)
    return (quant, scale, attended)

def reference(kv_cache, queries, fresh_key_value, lengths):
    quant, scale, attended = lax.map(lambda items: one_layer(lengths, items), (kv_cache, queries, fresh_key_value))
    return (quant, scale, attended)
```

```python
import functools
import math

import jax
import jax.numpy as jnp
from jax import lax
from jax.experimental import pallas as pl
from jax.experimental.pallas import tpu as pltpu
from jax.sharding import PartitionSpec as P

HEAD_DIM = 128
QUERY_GROUP = 8
BLOCK = 128
NEG = -1e30


def partner(me, step, count):
    if count & (count - 1) == 0:
        return me ^ step
    return (me + step) % count


def source(me, step, count):
    if count & (count - 1) == 0:
        return me ^ step
    return (me + count - step) % count


def cost(flops, nbytes):
    return pl.CostEstimate(flops=flops, bytes_accessed=nbytes, transcendentals=0)


def params(**kw):
    return pltpu.CompilerParams(vmem_limit_bytes=40 * 2**20, **kw)


def prep_kernel(place, *refs):
    half = len(refs) // 2
    for src, dst in zip(refs[:half], refs[half:]):
        dst[...] = src[0, 0]


def prepare(kv_cache, place, layer, which, low, number, count):
    _, _, batch, rows, width = kv_cache.shape
    pairs = width // HEAD_DIM * batch // count
    per = math.gcd(number, low, batch, 4)

    def where(step):
        def index(i, place):
            peer = partner(place[0], step, count)
            first = peer * pairs + low + i * per
            return (layer, which, (first % batch) // per, 0, first // batch)

        return index

    steps = range(1, count)
    piece = jax.ShapeDtypeStruct((number, rows, HEAD_DIM), kv_cache.dtype)
    return pl.pallas_call(
        prep_kernel,
        grid_spec=pltpu.PrefetchScalarGridSpec(
            num_scalar_prefetch=1,
            grid=(number // per,),
            in_specs=[pl.BlockSpec((1, 1, per, rows, HEAD_DIM), where(s)) for s in steps],
            out_specs=[pl.BlockSpec((per, rows, HEAD_DIM), lambda i, place: (i, 0, 0)) for s in steps],
        ),
        out_shape=[piece for _ in steps],
        cost_estimate=cost(10**7, 4 * number * rows * HEAD_DIM * count),
        compiler_params=params(),
        name="prepare",
    )(place, *[kv_cache for _ in steps])


def gather_pair(place, pieces, raw, j, rows, count):
    for step, piece in enumerate(pieces):
        at = source(place[0], step, count) * rows
        values = piece[0, 0, j] if step == 0 else piece[j]
        raw[pl.ds(pl.multiple_of(at, rows), rows), :] = values


def quantize(raw, out, j, n):
    at = pl.ds(n * BLOCK, BLOCK)
    values = raw[at, :].astype(jnp.float32)
    high = jnp.maximum(jnp.max(jnp.abs(values), axis=(0, 1), keepdims=True), 1.0)
    quant = (values * (127.0 / high)).astype(jnp.bfloat16)
    out[0, 0, j, at, :] = quant
    return high / 127.0, quant


def key_kernel(low, batch, blocks, count, place, lengths, own, *refs):
    pieces = (own,) + refs[: count - 1]
    query = refs[count - 1]
    quant_out, scale_out, weight_out, stat_out, summary_out, raw = refs[-6:]
    per, rows = own.shape[2], own.shape[3]
    pairs = scale_out.shape[2]
    step = pl.program_id(0)
    lane = lax.broadcasted_iota(jnp.int32, (QUERY_GROUP, BLOCK), 1)
    inverse = 1.0 / math.sqrt(HEAD_DIM)
    for j in range(per):
        gather_pair(place, pieces, raw.at[j], j, rows, count)
        pair = low + step * per + j
        live = lengths[(place[0] * pairs + pair) % batch] - place[1] * (rows * count)
        scales = jnp.zeros((1, BLOCK), jnp.float32)
        peaks = jnp.full((QUERY_GROUP, BLOCK), NEG, jnp.float32)
        totals = jnp.zeros((QUERY_GROUP, BLOCK), jnp.float32)
        for n in range(blocks):
            scale, quant = quantize(raw.at[j], quant_out, j, n)
            scales = jnp.where(lane[:1] == n, scale, scales)
            score = lax.dot_general(
                query[0, j], quant, (((1,), (1,)), ((), ())), preferred_element_type=jnp.float32
            )
            valid = lane + n * BLOCK < live
            masked = jnp.where(valid, score * scale * inverse, NEG)
            peak = jnp.max(masked, axis=1, keepdims=True)
            weight = jnp.where(valid, jnp.exp(masked - peak), 0.0)
            weight_out[j, :, pl.ds(n * BLOCK, BLOCK)] = weight
            peaks = jnp.where(lane == n, peak, peaks)
            totals = jnp.where(lane == n, jnp.sum(weight, axis=1, keepdims=True), totals)
        scale_out[0, 0, pl.ds(pair, 1), :] = scales[:, :blocks]
        stat_out[j] = peaks
        top = jnp.max(peaks, axis=1, keepdims=True)
        total = jnp.sum(jnp.exp(peaks - top) * totals, axis=1, keepdims=True)
        summary_out[j] = jnp.where(lane == 0, top, total)


def value_kernel(low, batch, blocks, count, place, lengths, own, *refs):
    pieces = (own,) + refs[: count - 1]
    weight_in, stat_in, plan_in = refs[count - 1 : count + 2]
    quant_out, scale_out, sum_out, raw = refs[-4:]
    per, rows = own.shape[2], own.shape[3]
    step = pl.program_id(0)
    lane = lax.broadcasted_iota(jnp.int32, (1, BLOCK), 1)
    for j in range(per):
        gather_pair(place, pieces, raw.at[j], j, rows, count)
        pair = low + step * per + j
        scales = jnp.zeros((1, BLOCK), jnp.float32)
        factor = jnp.exp(stat_in[j] - plan_in[j, :, :1]) / plan_in[j, :, 1:2]
        numer = jnp.zeros((QUERY_GROUP, HEAD_DIM), jnp.float32)
        for n in range(blocks):
            scale, quant = quantize(raw.at[j], quant_out, j, n)
            scales = jnp.where(lane == n, scale, scales)
            weight = (weight_in[j, :, pl.ds(n * BLOCK, BLOCK)] * scale).astype(jnp.bfloat16)
            part = jnp.dot(weight, quant, preferred_element_type=jnp.float32)
            numer = numer + factor[:, n : n + 1] * part
        scale_out[0, 0, pl.ds(pair, 1), :] = scales[:, :blocks]
        sum_out[j] = numer


def consume(kernel, kv_cache, pieces, place, lengths, extra, outs, held, layer, which, low, number, count):
    layers, _, batch, rows, width = kv_cache.shape
    pairs = width // HEAD_DIM * batch // count
    seq_rows = rows * count
    blocks = seq_rows // BLOCK
    per = math.gcd(number, low, 2)

    def mine(i, place, lengths):
        first = place[0] * pairs + low + i * per
        return (layer, which, (first % batch) // per, 0, first // batch)

    def big(i, place, lengths):
        return (layer, which, low // per + i, 0, 0)

    def rest(shape, layered):
        if layered:
            return pl.BlockSpec((1, per, *shape[2:]), lambda i, a, b: (layer, low // per + i, *[0] * (len(shape) - 2)))
        return pl.BlockSpec((per, *shape[1:]), lambda i, a, b: (low // per + i, *[0] * (len(shape) - 1)))

    in_specs = [pl.BlockSpec((1, 1, per, rows, HEAD_DIM), mine)]
    in_specs += [pl.BlockSpec((per, rows, HEAD_DIM), lambda i, place, lengths: (i, 0, 0)) for _ in pieces]
    in_specs += [rest(x.shape, x.ndim == 4) for x in extra]
    operands = [kv_cache, *pieces, *extra]
    aliases = {}
    for at, array in enumerate(held):
        if array is not None:
            aliases[2 + len(operands)] = at
            in_specs.append(pl.BlockSpec(memory_space=pl.ANY))
            operands.append(array)
    return pl.pallas_call(
        functools.partial(kernel, low, batch, blocks, count),
        grid_spec=pltpu.PrefetchScalarGridSpec(
            num_scalar_prefetch=2,
            grid=(number // per,),
            in_specs=in_specs,
            out_specs=[
                pl.BlockSpec((1, 1, per, seq_rows, HEAD_DIM), big),
                pl.BlockSpec((1, 1, pairs, blocks), lambda i, place, lengths: (layer, which, 0, 0)),
                *[rest(x.shape, False) for x in outs],
            ],
            scratch_shapes=[pltpu.VMEM((per, seq_rows, HEAD_DIM), jnp.bfloat16)],
        ),
        out_shape=[
            jax.ShapeDtypeStruct((layers, 2, pairs, seq_rows, HEAD_DIM), jnp.bfloat16),
            jax.ShapeDtypeStruct((layers, 2, pairs, blocks), jnp.float32),
            *outs,
        ],
        input_output_aliases=aliases,
        cost_estimate=cost(10**7, 4 * number * seq_rows * HEAD_DIM),
        compiler_params=params(),
    )(place, lengths, *operands)


def tree(join, values):
    while len(values) > 1:
        values = [join(*values[i : i + 2]) if i + 1 < len(values) else values[i] for i in range(0, len(values), 2)]
    return values[0]


def plan_kernel(query, fresh, *refs):
    summaries, plan_out, term_out = refs[:-2], refs[-2], refs[-1]
    lane = lax.broadcasted_iota(jnp.int32, (1, 1, BLOCK), 2)
    own = jnp.sum(
        query[0].astype(jnp.float32) * fresh[0, 0].astype(jnp.float32)[:, None, :], axis=-1, keepdims=True
    ) * (1.0 / math.sqrt(HEAD_DIM))
    top = jnp.maximum(tree(jnp.maximum, [s[:, :, :1] for s in summaries]), own)
    own_weight = jnp.exp(own - top)
    denom = tree(jnp.add, [jnp.exp(s[:, :, :1] - top) * s[:, :, 1:2] for s in summaries]) + own_weight
    plan_out[...] = jnp.where(lane == 0, top, denom)
    term_out[...] = own_weight / denom * fresh[0, 1].astype(jnp.float32)[:, None, :]


def make_plan(grouped, fresh, summaries, layer):
    pairs = grouped.shape[1]
    shape = (pairs, QUERY_GROUP, HEAD_DIM)
    whole = pl.BlockSpec(shape, lambda i: (0, 0, 0))
    return pl.pallas_call(
        plan_kernel,
        grid=(1,),
        in_specs=[
            pl.BlockSpec((1, *shape), lambda i: (layer, 0, 0, 0)),
            pl.BlockSpec((1, 2, pairs, HEAD_DIM), lambda i: (layer, 0, 0, 0)),
            *[whole for _ in summaries],
        ],
        out_specs=[whole, whole],
        out_shape=[jax.ShapeDtypeStruct(shape, jnp.float32)] * 2,
        cost_estimate=cost(10**6, 10**6),
        compiler_params=params(),
        name="plan",
    )(grouped, fresh, *summaries)


def finish_kernel(members, term, *refs):
    out = refs[-1]
    result = tree(jnp.add, [s[...] for s in refs[:members]]) + term[...]
    for g in range(QUERY_GROUP):
        out[0, :, g * HEAD_DIM : (g + 1) * HEAD_DIM] = result[:, g, :].astype(jnp.bfloat16)


def finish(term, shares, held, layer, layers):
    pairs = term.shape[0]
    width = QUERY_GROUP * HEAD_DIM
    whole = pl.BlockSpec(term.shape, lambda i: (0, 0, 0))
    operands = [term, *shares]
    in_specs = [whole for _ in operands]
    aliases = {}
    if held is not None:
        aliases = {len(operands): 0}
        in_specs.append(pl.BlockSpec(memory_space=pl.ANY))
        operands.append(held)
    return pl.pallas_call(
        functools.partial(finish_kernel, len(shares)),
        grid=(1,),
        in_specs=in_specs,
        out_specs=pl.BlockSpec((1, pairs, width), lambda i: (layer, 0, 0)),
        out_shape=jax.ShapeDtypeStruct((layers, pairs, width), jnp.bfloat16),
        input_output_aliases=aliases,
        cost_estimate=cost(10**6, 10**6),
        compiler_params=params(),
        name="finish",
    )(*operands)


def chunks_of(layers, pairs):
    chunks = [(layer, which, 0, pairs) for layer in range(layers) for which in (0, 1)]
    if pairs % 16 == 0:
        quarter = pairs // 4
        chunks[-1:] = [
            (layers - 1, 1, 0, 2 * quarter),
            (layers - 1, 1, 2 * quarter, quarter),
            (layers - 1, 1, 3 * quarter, quarter),
        ]
    return chunks


def by_pieces(kv_cache, queries, fresh, lengths):
    layers, _, batch, rows, width = kv_cache.shape
    count = lax.axis_size("blk")
    members = lax.axis_size("seq")
    pairs = width // HEAD_DIM * batch // count
    seq_rows = rows * count
    place = jnp.stack([lax.axis_index("blk"), lax.axis_index("seq")]).astype(jnp.int32)
    grouped = queries.reshape(layers, pairs, QUERY_GROUP, HEAD_DIM)
    small = jax.ShapeDtypeStruct((pairs, QUERY_GROUP, HEAD_DIM), jnp.float32)
    weight_shape = jax.ShapeDtypeStruct((pairs, QUERY_GROUP, seq_rows), jnp.float32)

    def share(array):
        shared = [array]
        for step in range(1, members):
            ring = [(me, partner(me, step, members)) for me in range(members)]
            shared.append(lax.ppermute(array, "seq", ring))
        return shared

    held = [None, None]
    attended = None
    for layer, which, low, number in chunks_of(layers, pairs):
        sent = prepare(kv_cache, place, layer, which, low, number, count)
        pieces = [None] * (count - 1)
        for step in range(1, count):
            ring = [(me, partner(me, step, count)) for me in range(count)]
            pieces[step - 1] = lax.ppermute(sent[step - 1], "blk", ring)
        common = (kv_cache, pieces, place, lengths)
        chunk = (layer, which, low, number, count)
        last = low + number == pairs
        if which == 0:
            inner = [None] * 3 if low == 0 else inner
            results = consume(
                key_kernel, *common, (grouped,), (weight_shape, small, small), held + inner, *chunk
            )
            held, inner = list(results[:2]), list(results[2:])
            if last:
                weights, stats, summary = inner
                summaries = share(summary)
                plan, term = make_plan(grouped, fresh, summaries, layer)
            continue
        inner = [None] if low == 0 else inner
        results = consume(
            value_kernel, *common, (weights, stats, plan), (small,), held + inner, *chunk
        )
        held, inner = list(results[:2]), list(results[2:])
        if last:
            shares = share(inner[0])
            attended = finish(term, shares, attended, layer, layers)
    return (*held, attended)


def by_all_to_all(kv_cache, queries, fresh_key_value, lengths):
    layers, _, batch, local_rows, width = kv_cache.shape
    heads = width // HEAD_DIM
    blk_count = lax.axis_size("blk")
    blk_place = lax.axis_index("blk")
    pairs_here = heads * batch // blk_count
    seq_rows = local_rows * blk_count
    blocks_here = seq_rows // BLOCK
    arranged = kv_cache.reshape(layers, 2, batch, local_rows, heads, HEAD_DIM).transpose(
        0, 1, 4, 2, 3, 5
    )
    arranged = arranged.reshape(layers, 2, heads * batch, local_rows, HEAD_DIM)
    pair_start = blk_place * pairs_here
    moved = lax.all_to_all(arranged, "blk", split_axis=2, concat_axis=3, tiled=True)
    grouped = moved.reshape(layers, 2, pairs_here, blocks_here, BLOCK, HEAD_DIM)
    block_scale = (
        jnp.maximum(jnp.max(jnp.abs(grouped), axis=(4, 5)).astype(jnp.float32), 1.0) / 127.0
    )
    quant = (grouped.astype(jnp.float32) / block_scale[..., None, None]).astype(jnp.bfloat16)
    quant = quant.reshape(layers, 2, pairs_here, seq_rows, HEAD_DIM)
    seq_start = lax.axis_index("seq") * seq_rows
    pair_len = lax.dynamic_slice_in_dim(jnp.tile(lengths, heads), pair_start, pairs_here)
    positions = seq_start + jnp.arange(seq_rows, dtype=jnp.int32).reshape(blocks_here, BLOCK)
    valid = positions[None] < pair_len[:, None, None]
    inverse = 1.0 / jnp.sqrt(jnp.float32(HEAD_DIM))
    grouped_queries = queries.reshape(layers, pairs_here, QUERY_GROUP, HEAD_DIM)
    peaks = []
    totals = []
    sums = []
    for layer in range(layers):
        raw = jnp.einsum(
            "pgd,prd->pgr",
            grouped_queries[layer],
            quant[layer, 0],
            preferred_element_type=jnp.float32,
        )
        scores = (
            raw.reshape(pairs_here, QUERY_GROUP, blocks_here, BLOCK)
            * block_scale[layer, 0][:, None, :, None]
            * inverse
        )
        masked = jnp.where(valid[:, None], scores, -1e30)
        block_top = jnp.max(masked, axis=-1)
        weight = jnp.where(valid[:, None], jnp.exp(masked - block_top[..., None]), 0.0)
        block_total = jnp.sum(weight, axis=-1)
        rounded = (weight * block_scale[layer, 1][:, None, :, None]).astype(jnp.bfloat16)
        values = quant[layer, 1].reshape(pairs_here, blocks_here, BLOCK, HEAD_DIM)
        block_sum = jnp.einsum(
            "pgnt,pntd->pgnd", rounded, values, preferred_element_type=jnp.float32
        )
        local_top = jnp.max(block_top, axis=-1)
        scale_factor = jnp.exp(block_top - local_top[..., None])
        peaks.append(local_top)
        totals.append(jnp.sum(scale_factor * block_total, axis=-1))
        sums.append(jnp.sum(scale_factor[..., None] * block_sum, axis=2))
    peak = jnp.stack(peaks)
    total = jnp.stack(totals)
    weighted = jnp.stack(sums)
    shared_top = lax.pmax(peak, "seq")
    scale_factor = jnp.exp(peak - shared_top)
    total, weighted = lax.psum((total * scale_factor, weighted * scale_factor[..., None]), "seq")
    peak = shared_top
    own = (
        jnp.einsum(
            "lpgd,lpd->lpg",
            grouped_queries,
            fresh_key_value[:, 0],
            preferred_element_type=jnp.float32,
        )
        * inverse
    )
    top = jnp.maximum(peak, own)
    cache_w = jnp.exp(peak - top)
    own_w = jnp.exp(own - top)
    numer = (
        weighted * cache_w[..., None]
        + own_w[..., None] * fresh_key_value[:, 1].astype(jnp.float32)[:, :, None, :]
    )
    denom = total * cache_w + own_w
    attended = (
        (numer / denom[..., None])
        .reshape(layers, pairs_here, QUERY_GROUP * HEAD_DIM)
        .astype(jnp.bfloat16)
    )
    return (quant, block_scale, attended)


def on_device(kv_cache, queries, fresh_key_value, lengths):
    exchange = by_pieces if by_blocks(kv_cache.shape[3]) else by_all_to_all
    return exchange(kv_cache, queries, fresh_key_value, lengths)


def by_blocks(local_rows):
    return local_rows % BLOCK == 0


def solution(mesh):
    in_specs = (
        P(None, None, None, ("seq", "blk"), None),
        P(None, "blk", None),
        P(None, None, "blk", None),
        P(),
    )
    out_specs = (
        P(None, None, "blk", "seq", None),
        P(None, None, "blk", "seq"),
        P(None, "blk", None),
    )

    def program(kv_cache, queries, fresh_key_value, lengths):
        step = jax.shard_map(
            on_device, mesh=mesh, in_specs=in_specs, out_specs=out_specs, check_vma=False
        )
        return step(kv_cache, queries, fresh_key_value, lengths)

    return program
```

```python
import functools
import math

import jax
import jax.numpy as jnp
from jax import lax
from jax.experimental import pallas as pl
from jax.experimental.pallas import tpu as pltpu
from jax.sharding import PartitionSpec as P

HEAD_DIM = 128
QUERY_GROUP = 8
BLOCK = 128
NEG = -1e30


def turn(me, step, count):
    quarter = count // 4
    far = 3 * quarter
    if quarter < 2 or step not in (1, far):
        return step
    middle = (me // quarter + 1) // 2 % 2
    return 1 + middle * (far - 1) if step == 1 else far - middle * (far - 1)


def partner(me, step, count):
    if count & (count - 1) == 0:
        return me ^ turn(me, step, count)
    return (me + step) % count


def source(me, step, count):
    if count & (count - 1) == 0:
        return me ^ turn(me, step, count)
    return (me + count - step) % count


def cost(flops, nbytes):
    return pl.CostEstimate(flops=flops, bytes_accessed=nbytes, transcendentals=0)


def params(**kw):
    return pltpu.CompilerParams(vmem_limit_bytes=40 * 2**20, **kw)


def prep_kernel(place, *refs):
    half = len(refs) // 2
    for src, dst in zip(refs[:half], refs[half:]):
        dst[...] = src[0, 0]


def prepare(kv_cache, place, layer, which, low, number, count, steps):
    _, _, batch, rows, width = kv_cache.shape
    pairs = width // HEAD_DIM * batch // count
    per = math.gcd(number, low, batch, 8 if len(steps) < 3 else 4)

    def where(step):
        def index(i, place):
            peer = partner(place[0], step, count)
            first = peer * pairs + low + i * per
            return (layer, which, (first % batch) // per, 0, first // batch)

        return index

    piece = jax.ShapeDtypeStruct((number, rows, HEAD_DIM), kv_cache.dtype)
    return pl.pallas_call(
        prep_kernel,
        grid_spec=pltpu.PrefetchScalarGridSpec(
            num_scalar_prefetch=1,
            grid=(number // per,),
            in_specs=[pl.BlockSpec((1, 1, per, rows, HEAD_DIM), where(s)) for s in steps],
            out_specs=[pl.BlockSpec((per, rows, HEAD_DIM), lambda i, place: (i, 0, 0)) for s in steps],
        ),
        out_shape=[piece for _ in steps],
        cost_estimate=cost(10**7, 4 * number * rows * HEAD_DIM * len(steps)),
        compiler_params=params(),
        name="prepare",
    )(place, *[kv_cache for _ in steps])


def gather_pair(place, pieces, raw, j, rows, count):
    for step, piece in enumerate(pieces):
        at = source(place[0], step, count) * rows
        values = piece[0, 0, j] if step == 0 else piece[j]
        raw[pl.ds(pl.multiple_of(at, rows), rows), :] = values


def quantize(raw, out, j, n):
    at = pl.ds(n * BLOCK, BLOCK)
    values = raw[at, :].astype(jnp.float32)
    high = jnp.maximum(jnp.max(jnp.abs(values), axis=(0, 1), keepdims=True), 1.0)
    quant = (values * (127.0 / high)).astype(jnp.bfloat16)
    out[0, 0, j, at, :] = quant
    return high / 127.0, quant


def key_kernel(low, batch, blocks, count, place, lengths, own, *refs):
    pieces = (own,) + refs[: count - 1]
    query = refs[count - 1]
    quant_out, scale_out, weight_out, stat_out, summary_out, raw = refs[-6:]
    per, rows = own.shape[2], own.shape[3]
    pairs = scale_out.shape[2]
    step = pl.program_id(0)
    lane = lax.broadcasted_iota(jnp.int32, (QUERY_GROUP, BLOCK), 1)
    inverse = 1.0 / math.sqrt(HEAD_DIM)
    for j in range(per):
        gather_pair(place, pieces, raw.at[j], j, rows, count)
        pair = low + step * per + j
        live = lengths[(place[0] * pairs + pair) % batch] - place[1] * (rows * count)
        scales = jnp.zeros((1, BLOCK), jnp.float32)
        peaks = jnp.full((QUERY_GROUP, BLOCK), NEG, jnp.float32)
        totals = jnp.zeros((QUERY_GROUP, BLOCK), jnp.float32)
        for n in range(blocks):
            scale, quant = quantize(raw.at[j], quant_out, j, n)
            scales = jnp.where(lane[:1] == n, scale, scales)
            score = lax.dot_general(
                query[0, j], quant, (((1,), (1,)), ((), ())), preferred_element_type=jnp.float32
            )
            valid = lane + n * BLOCK < live
            masked = jnp.where(valid, score * scale * inverse, NEG)
            peak = jnp.max(masked, axis=1, keepdims=True)
            weight = jnp.where(valid, jnp.exp(masked - peak), 0.0)
            weight_out[j, :, pl.ds(n * BLOCK, BLOCK)] = weight
            peaks = jnp.where(lane == n, peak, peaks)
            totals = jnp.where(lane == n, jnp.sum(weight, axis=1, keepdims=True), totals)
        scale_out[0, 0, pl.ds(pair, 1), :] = scales[:, :blocks]
        stat_out[j] = peaks
        top = jnp.max(peaks, axis=1, keepdims=True)
        total = jnp.sum(jnp.exp(peaks - top) * totals, axis=1, keepdims=True)
        summary_out[j] = jnp.where(lane == 0, top, total)


def value_kernel(low, batch, blocks, count, place, lengths, own, *refs):
    pieces = (own,) + refs[: count - 1]
    weight_in, stat_in, plan_in = refs[count - 1 : count + 2]
    quant_out, scale_out, sum_out, raw = refs[-4:]
    per, rows = own.shape[2], own.shape[3]
    step = pl.program_id(0)
    lane = lax.broadcasted_iota(jnp.int32, (1, BLOCK), 1)
    for j in range(per):
        gather_pair(place, pieces, raw.at[j], j, rows, count)
        pair = low + step * per + j
        scales = jnp.zeros((1, BLOCK), jnp.float32)
        factor = jnp.exp(stat_in[j] - plan_in[j, :, :1]) / plan_in[j, :, 1:2]
        numer = jnp.zeros((QUERY_GROUP, HEAD_DIM), jnp.float32)
        for n in range(blocks):
            scale, quant = quantize(raw.at[j], quant_out, j, n)
            scales = jnp.where(lane == n, scale, scales)
            weight = (weight_in[j, :, pl.ds(n * BLOCK, BLOCK)] * scale).astype(jnp.bfloat16)
            part = jnp.dot(weight, quant, preferred_element_type=jnp.float32)
            numer = numer + factor[:, n : n + 1] * part
        scale_out[0, 0, pl.ds(pair, 1), :] = scales[:, :blocks]
        sum_out[j] = numer


def consume(kernel, kv_cache, pieces, place, lengths, extra, outs, held, layer, which, low, number, base, count):
    layers, _, batch, rows, width = kv_cache.shape
    pairs = width // HEAD_DIM * batch // count
    seq_rows = rows * count
    blocks = seq_rows // BLOCK
    per = math.gcd(number, low, 2)

    def mine(i, place, lengths):
        first = place[0] * pairs + low + i * per
        return (layer, which, (first % batch) // per, 0, first // batch)

    def big(i, place, lengths):
        return (layer, which, low // per + i, 0, 0)

    def rest(shape, first):
        ahead = (layer,) if len(shape) == 4 else ()
        tail = shape[len(ahead) + 1 :]
        return pl.BlockSpec(
            (*[1 for _ in ahead], per, *tail), lambda i, a, b: (*ahead, first // per + i, *[0 for _ in tail])
        )

    in_specs = [pl.BlockSpec((1, 1, per, rows, HEAD_DIM), mine)]
    in_specs += [pl.BlockSpec((per, rows, HEAD_DIM), lambda i, place, lengths: (i, 0, 0)) for _ in pieces]
    in_specs += [rest(x.shape, low) for x in extra]
    operands = [kv_cache, *pieces, *extra]
    aliases = {}
    for at, array in enumerate(held):
        if array is not None:
            aliases[2 + len(operands)] = at
            in_specs.append(pl.BlockSpec(memory_space=pl.ANY))
            operands.append(array)
    return pl.pallas_call(
        functools.partial(kernel, low, batch, blocks, count),
        grid_spec=pltpu.PrefetchScalarGridSpec(
            num_scalar_prefetch=2,
            grid=(number // per,),
            in_specs=in_specs,
            out_specs=[
                pl.BlockSpec((1, 1, per, seq_rows, HEAD_DIM), big),
                pl.BlockSpec((1, 1, pairs, blocks), lambda i, place, lengths: (layer, which, 0, 0)),
                *[rest(x.shape, low - base) for x in outs],
            ],
            scratch_shapes=[pltpu.VMEM((per, seq_rows, HEAD_DIM), jnp.bfloat16)],
        ),
        out_shape=[
            jax.ShapeDtypeStruct((layers, 2, pairs, seq_rows, HEAD_DIM), jnp.bfloat16),
            jax.ShapeDtypeStruct((layers, 2, pairs, blocks), jnp.float32),
            *outs,
        ],
        input_output_aliases=aliases,
        cost_estimate=cost(10**7, 4 * number * seq_rows * HEAD_DIM),
        compiler_params=params(),
    )(place, lengths, *operands)


def tree(join, values):
    while len(values) > 1:
        values = [join(*values[i : i + 2]) if i + 1 < len(values) else values[i] for i in range(0, len(values), 2)]
    return values[0]


def plan_kernel(query, fresh, *refs):
    summaries, plan_out, term_out = refs[:-2], refs[-2], refs[-1]
    lane = lax.broadcasted_iota(jnp.int32, (1, 1, BLOCK), 2)
    own = jnp.sum(
        query[0].astype(jnp.float32) * fresh[0, 0].astype(jnp.float32)[:, None, :], axis=-1, keepdims=True
    ) * (1.0 / math.sqrt(HEAD_DIM))
    top = jnp.maximum(tree(jnp.maximum, [s[:, :, :1] for s in summaries]), own)
    own_weight = jnp.exp(own - top)
    denom = tree(jnp.add, [jnp.exp(s[:, :, :1] - top) * s[:, :, 1:2] for s in summaries]) + own_weight
    plan_out[...] = jnp.where(lane == 0, top, denom)
    term_out[...] = own_weight / denom * fresh[0, 1].astype(jnp.float32)[:, None, :]


def make_plan(grouped, fresh, summaries, layer):
    pairs = grouped.shape[1]
    shape = (pairs, QUERY_GROUP, HEAD_DIM)
    whole = pl.BlockSpec(shape, lambda i: (0, 0, 0))
    return pl.pallas_call(
        plan_kernel,
        grid=(1,),
        in_specs=[
            pl.BlockSpec((1, *shape), lambda i: (layer, 0, 0, 0)),
            pl.BlockSpec((1, 2, pairs, HEAD_DIM), lambda i: (layer, 0, 0, 0)),
            *[whole for _ in summaries],
        ],
        out_specs=[whole, whole],
        out_shape=[jax.ShapeDtypeStruct(shape, jnp.float32)] * 2,
        cost_estimate=cost(10**6, 10**6),
        compiler_params=params(),
        name="plan",
    )(grouped, fresh, *summaries)


def merge_kernel(*refs):
    refs[-1][...] = tree(jnp.add, [s[...] for s in refs[:-1]])


def merge(shares):
    whole = pl.BlockSpec(shares[0].shape, lambda i: (0, 0, 0))
    return pl.pallas_call(
        merge_kernel,
        grid=(1,),
        in_specs=[whole for _ in shares],
        out_specs=whole,
        out_shape=jax.ShapeDtypeStruct(shares[0].shape, jnp.float32),
        cost_estimate=cost(10**6, 10**6),
        compiler_params=params(),
        name="merge",
    )(*shares)


def finish_kernel(members, merged, term, *refs):
    out = refs[-1]
    shared = tree(jnp.add, [s[...] for s in refs[:members]])
    result = jnp.concatenate([*(s[...] for s in refs[members : members + merged]), shared], axis=0) + term[...]
    for g in range(QUERY_GROUP):
        out[0, :, g * HEAD_DIM : (g + 1) * HEAD_DIM] = result[:, g, :].astype(jnp.bfloat16)


def finish(term, shares, merged, held, layer, layers):
    pairs = term.shape[0]
    width = QUERY_GROUP * HEAD_DIM
    operands = [term, *shares, *merged]
    in_specs = [pl.BlockSpec(x.shape, lambda i: (0, 0, 0)) for x in operands]
    aliases = {}
    if held is not None:
        aliases = {len(operands): 0}
        in_specs.append(pl.BlockSpec(memory_space=pl.ANY))
        operands.append(held)
    return pl.pallas_call(
        functools.partial(finish_kernel, len(shares), len(merged)),
        grid=(1,),
        in_specs=in_specs,
        out_specs=pl.BlockSpec((1, pairs, width), lambda i: (layer, 0, 0)),
        out_shape=jax.ShapeDtypeStruct((layers, pairs, width), jnp.bfloat16),
        input_output_aliases=aliases,
        cost_estimate=cost(10**6, 10**6),
        compiler_params=params(),
        name="finish",
    )(*operands)


def chunks_of(layers, pairs):
    chunks = [(layer, which, 0, pairs, 0, pairs) for layer in range(layers) for which in (0, 1)]
    if pairs % 16 == 0:
        quarter = pairs // 4
        chunks[-1:] = [
            (layers - 1, 1, 0, 2 * quarter, 0, 3 * quarter),
            (layers - 1, 1, 2 * quarter, quarter, 0, 3 * quarter),
            (layers - 1, 1, 3 * quarter, quarter, 3 * quarter, pairs),
        ]
    return chunks


def order_of(at, count):
    half = count // 2
    if count < 8:
        return list(range(1, count))
    near, far = list(range(2, half)), list(range(half, count - 1))
    return [1, *near, count - 1, *far] if at else [1, count - 1, *near, *far]


def parts_of(at, count):
    order = order_of(at, count)
    return [order] if at else [order[:2], order[2:]]


def by_pieces(kv_cache, queries, fresh, lengths):
    layers, _, batch, rows, width = kv_cache.shape
    count = lax.axis_size("blk")
    members = lax.axis_size("seq")
    pairs = width // HEAD_DIM * batch // count
    seq_rows = rows * count
    place = jnp.stack([lax.axis_index("blk"), lax.axis_index("seq")]).astype(jnp.int32)
    grouped = queries.reshape(layers, pairs, QUERY_GROUP, HEAD_DIM)
    small = jax.ShapeDtypeStruct((pairs, QUERY_GROUP, HEAD_DIM), jnp.float32)
    weight_shape = jax.ShapeDtypeStruct((pairs, QUERY_GROUP, seq_rows), jnp.float32)

    def share(array):
        shared = [array]
        for step in range(1, members):
            ring = [(me, partner(me, step, members)) for me in range(members)]
            shared.append(lax.ppermute(array, "seq", ring))
        return shared

    held = [None, None]
    attended = None
    merged = []
    for at, (layer, which, low, number, base, end) in enumerate(chunks_of(layers, pairs)):
        pieces = [None] * (count - 1)
        for steps in parts_of(at, count):
            sent = prepare(kv_cache, place, layer, which, low, number, count, steps)
            for step, piece in zip(steps, sent):
                ring = [(me, partner(me, step, count)) for me in range(count)]
                pieces[step - 1] = lax.ppermute(piece, "blk", ring)
        common = (kv_cache, pieces, place, lengths)
        chunk = (layer, which, low, number, base, count)
        if which == 0:
            inner = [None] * 3 if low == base else inner
            results = consume(
                key_kernel, *common, (grouped,), (weight_shape, small, small), held + inner, *chunk
            )
            held, inner = list(results[:2]), list(results[2:])
            if low + number == end:
                weights, stats, summary = inner
                summaries = share(summary)
                plan, term = make_plan(grouped, fresh, summaries, layer)
            continue
        inner = [None] if low == base else inner
        sums = jax.ShapeDtypeStruct((end - base, QUERY_GROUP, HEAD_DIM), jnp.float32)
        results = consume(
            value_kernel, *common, (weights, stats, plan), (sums,), held + inner, *chunk
        )
        held, inner = list(results[:2]), list(results[2:])
        if low + number == end:
            shares = share(inner[0])
            if end < pairs:
                merged.append(merge(shares))
                continue
            attended = finish(term, shares, merged, attended, layer, layers)
            merged = []
    return (*held, attended)


def by_all_to_all(kv_cache, queries, fresh_key_value, lengths):
    layers, _, batch, local_rows, width = kv_cache.shape
    heads = width // HEAD_DIM
    blk_count = lax.axis_size("blk")
    blk_place = lax.axis_index("blk")
    pairs_here = heads * batch // blk_count
    seq_rows = local_rows * blk_count
    blocks_here = seq_rows // BLOCK
    arranged = kv_cache.reshape(layers, 2, batch, local_rows, heads, HEAD_DIM).transpose(
        0, 1, 4, 2, 3, 5
    )
    arranged = arranged.reshape(layers, 2, heads * batch, local_rows, HEAD_DIM)
    pair_start = blk_place * pairs_here
    moved = lax.all_to_all(arranged, "blk", split_axis=2, concat_axis=3, tiled=True)
    grouped = moved.reshape(layers, 2, pairs_here, blocks_here, BLOCK, HEAD_DIM)
    block_scale = (
        jnp.maximum(jnp.max(jnp.abs(grouped), axis=(4, 5)).astype(jnp.float32), 1.0) / 127.0
    )
    quant = (grouped.astype(jnp.float32) / block_scale[..., None, None]).astype(jnp.bfloat16)
    quant = quant.reshape(layers, 2, pairs_here, seq_rows, HEAD_DIM)
    seq_start = lax.axis_index("seq") * seq_rows
    pair_len = lax.dynamic_slice_in_dim(jnp.tile(lengths, heads), pair_start, pairs_here)
    positions = seq_start + jnp.arange(seq_rows, dtype=jnp.int32).reshape(blocks_here, BLOCK)
    valid = positions[None] < pair_len[:, None, None]
    inverse = 1.0 / jnp.sqrt(jnp.float32(HEAD_DIM))
    grouped_queries = queries.reshape(layers, pairs_here, QUERY_GROUP, HEAD_DIM)
    peaks = []
    totals = []
    sums = []
    for layer in range(layers):
        raw = jnp.einsum(
            "pgd,prd->pgr",
            grouped_queries[layer],
            quant[layer, 0],
            preferred_element_type=jnp.float32,
        )
        scores = (
            raw.reshape(pairs_here, QUERY_GROUP, blocks_here, BLOCK)
            * block_scale[layer, 0][:, None, :, None]
            * inverse
        )
        masked = jnp.where(valid[:, None], scores, -1e30)
        block_top = jnp.max(masked, axis=-1)
        weight = jnp.where(valid[:, None], jnp.exp(masked - block_top[..., None]), 0.0)
        block_total = jnp.sum(weight, axis=-1)
        rounded = (weight * block_scale[layer, 1][:, None, :, None]).astype(jnp.bfloat16)
        values = quant[layer, 1].reshape(pairs_here, blocks_here, BLOCK, HEAD_DIM)
        block_sum = jnp.einsum(
            "pgnt,pntd->pgnd", rounded, values, preferred_element_type=jnp.float32
        )
        local_top = jnp.max(block_top, axis=-1)
        scale_factor = jnp.exp(block_top - local_top[..., None])
        peaks.append(local_top)
        totals.append(jnp.sum(scale_factor * block_total, axis=-1))
        sums.append(jnp.sum(scale_factor[..., None] * block_sum, axis=2))
    peak = jnp.stack(peaks)
    total = jnp.stack(totals)
    weighted = jnp.stack(sums)
    shared_top = lax.pmax(peak, "seq")
    scale_factor = jnp.exp(peak - shared_top)
    total, weighted = lax.psum((total * scale_factor, weighted * scale_factor[..., None]), "seq")
    peak = shared_top
    own = (
        jnp.einsum(
            "lpgd,lpd->lpg",
            grouped_queries,
            fresh_key_value[:, 0],
            preferred_element_type=jnp.float32,
        )
        * inverse
    )
    top = jnp.maximum(peak, own)
    cache_w = jnp.exp(peak - top)
    own_w = jnp.exp(own - top)
    numer = (
        weighted * cache_w[..., None]
        + own_w[..., None] * fresh_key_value[:, 1].astype(jnp.float32)[:, :, None, :]
    )
    denom = total * cache_w + own_w
    attended = (
        (numer / denom[..., None])
        .reshape(layers, pairs_here, QUERY_GROUP * HEAD_DIM)
        .astype(jnp.bfloat16)
    )
    return (quant, block_scale, attended)


def on_device(kv_cache, queries, fresh_key_value, lengths):
    exchange = by_pieces if by_blocks(kv_cache.shape[3]) else by_all_to_all
    return exchange(kv_cache, queries, fresh_key_value, lengths)


def by_blocks(local_rows):
    return local_rows % BLOCK == 0


def solution(mesh):
    in_specs = (
        P(None, None, None, ("seq", "blk"), None),
        P(None, "blk", None),
        P(None, None, "blk", None),
        P(),
    )
    out_specs = (
        P(None, None, "blk", "seq", None),
        P(None, None, "blk", "seq"),
        P(None, "blk", None),
    )

    def program(kv_cache, queries, fresh_key_value, lengths):
        step = jax.shard_map(
            on_device, mesh=mesh, in_specs=in_specs, out_specs=out_specs, check_vma=False
        )
        return step(kv_cache, queries, fresh_key_value, lengths)

    return program
```
